32 devices in a mesh: patch: 32 (over z, y, x, core).
Axes of the slice: x: 2, y: 2, z: 4, core: 2. Of those that a mesh axis runs over, the one named last changes fastest.
Arguments:
- atm_flux: bfloat16 [8, 98304], P(None, 'patch'), may hold values from -6 to 6
- remap_send: int32 [32, 5, 8], P('patch'), may hold values from 0 to 23
- remap_target: int32 [32, 5, 8], P('patch'), may hold values from 0 to 31
- remap_counts: int32 [32, 5], P('patch'), may hold values from 0 to 8, as said below
- remap_weights: bfloat16 [32, 5, 8, 128, 128], P('patch'), may hold values from -0.5 to 0.5
- coupling: float32 [2, 8], replicated, may hold values from -2 to 2
- tracer: float32 [2, 128, 131072], P(None, None, 'patch'), may hold values from -6 to 6
- wet: int32 [131072], P('patch'), may hold values from 0 to 1
- mix_inverse: float32 [1024, 128, 128], P('patch')
- halo_send: int32 [32, 4, 2, 128], P('patch'), may hold values from 0 to 4095
- halo_ghost: int32 [32, 4, 2, 128], P('patch'), may hold values from 0 to 4095
- halo_rows: int32 [32, 4], P('patch'), may hold values from 0 to 2, as said below
Outputs:
- ocean_flux: float32 [8, 131072], P(None, 'patch')
- tracer_out: float32 [2, 128, 131072], P(None, None, 'patch')
The draws below stay inside these ranges and needn't reach their ends.
Inputs may be any that keep to these rules, and one draw needn't show every extreme that they name: `remap_counts`: some entry equals 8. `halo_rows`: some entry equals 2.
All inputs are finite; a program needn't handle non-finite values.
Results may differ from the reference program's by a relative error of at most 0.0003.
Values may be sent and summed in bfloat16 or wider, within the bound.
No kernel may reach another device: no remote copies, remote signals or barrier semaphores. Data moves between devices by JAX's collectives and lax.ppermute only.
A program may use at most 64 MiB of HBM per device.

```python
import math
import jax
import jax.numpy as jnp
from jax import lax

F = 8
LEV = 128
NTR = 2
BLOCK = 128
ABLK = 24
OBLK = 32
CAP = 8
REACH = 2
HR = 2
SPAN = 5
HSPAN = 4
OC = 4096
NOC = 131072
NA = 98304
N_PATCH = 32


def force_top(key, rows, columns, top):
    counts = jax.random.randint(jax.random.fold_in(key, 21), (rows * columns,), 0, top + 1)
    spot = jax.random.randint(jax.random.fold_in(key, 22), (), 0, rows * columns)
    counts = jnp.where(jnp.arange(rows * columns) == spot, top, counts)
    return counts.reshape(rows, columns).astype(jnp.int32)


def draw_remap_counts(key, part):
    return force_top(jax.random.fold_in(key, 31), N_PATCH, SPAN, CAP)


def draw_halo_rows(key, part):
    return force_top(jax.random.fold_in(key, 41), N_PATCH, HSPAN, HR)


def draw_wet(key, part):
    percent = jax.random.randint(jax.random.fold_in(key, 51), (N_PATCH, 1), 30, 96)
    rolled = jax.random.randint(jax.random.fold_in(key, 52), (N_PATCH, OBLK * BLOCK), 0, 100)
    return (rolled < percent).astype(jnp.int32).reshape(-1)


def draw_mix_inverse(key, part):
    count = N_PATCH * OBLK
    diag = jax.random.uniform(jax.random.fold_in(key, 61), (count, LEV, 1), jnp.float32, 0.6, 1.4)
    eye = jnp.eye(LEV, dtype=jnp.float32)[None, :, :]
    spread = 0.5 * jax.random.normal(jax.random.fold_in(key, 63), (count, LEV, LEV), jnp.float32)
    return (eye * diag + spread / math.sqrt(LEV)).astype(jnp.float32)


def plant(values, stream_key, low, largest):
    longest = values.shape.index(max(values.shape))
    spots = []
    for shift in (0, 1):
        where = [jax.random.randint(jax.random.fold_in(stream_key, axis), (), 0, length) for axis, length in enumerate(values.shape)]
        where[longest] = (where[longest] + shift) % values.shape[longest]
        spots.append(tuple(where))
    return values.at[spots[0]].set(low).at[spots[1]].set(largest)


def block_scale(own_key, extent, cuts, low, largest):
    loudness = 1.0
    for axis_at, shards_of in cuts:
        draws = jax.random.uniform(jax.random.fold_in(jax.random.fold_in(own_key, 6), axis_at), (shards_of,), jnp.float32, low / len(cuts), largest / len(cuts))
        loudness = loudness * jnp.repeat(jnp.exp(draws), extent[axis_at] // shards_of).reshape((-1,) + (1,) * (len(extent) - 1 - axis_at))
    return loudness


def centred(rng, shape, width, limit, split=(), kind=jnp.bfloat16):
    gain = block_scale(rng, shape, split, -0.22, 0.18) if split else 1.0
    drawn = jax.random.normal(rng, shape, jnp.float32) * width * gain
    return jnp.minimum(jnp.maximum(drawn, -limit), limit).astype(kind)


def setup_inputs(seed: int = 0) -> dict:
    key_of = jax.random.split(jax.random.key(seed), 13)
    atm_flux = centred(key_of[0], (F, NA), 1.0, 6.0, ((1, 32),))
    remap_send = plant(jax.random.randint(key_of[1], (N_PATCH, SPAN, CAP), 0, ABLK), jax.random.fold_in(key_of[1], 1), 0, ABLK - 1).astype(jnp.int32)
    remap_target = plant(jax.random.randint(key_of[2], (N_PATCH, SPAN, CAP), 0, OBLK), jax.random.fold_in(key_of[2], 1), 0, OBLK - 1).astype(jnp.int32)
    remap_counts = draw_remap_counts(jax.random.fold_in(key_of[12], 71), 0)
    remap_weights = centred(key_of[4], (N_PATCH, SPAN, CAP, BLOCK, BLOCK), BLOCK ** -0.5, 0.5, ((0, 32),))
    coupling = centred(key_of[5], (NTR, F), F ** -0.5, 2.0, (), jnp.float32)
    tracer = centred(key_of[6], (NTR, LEV, NOC), 1.0, 6.0, ((2, 32),), jnp.float32)
    wet = draw_wet(jax.random.fold_in(key_of[12], 71), 0)
    mix_inverse = draw_mix_inverse(jax.random.fold_in(key_of[12], 71), 0)
    halo_send = plant(jax.random.randint(key_of[9], (N_PATCH, HSPAN, HR, BLOCK), 0, OC), jax.random.fold_in(key_of[9], 1), 0, OC - 1).astype(jnp.int32)
    halo_ghost = plant(jax.random.randint(key_of[10], (N_PATCH, HSPAN, HR, BLOCK), 0, OC), jax.random.fold_in(key_of[10], 1), 0, OC - 1).astype(jnp.int32)
    halo_rows = draw_halo_rows(jax.random.fold_in(key_of[12], 71), 0)
    return dict(atm_flux=atm_flux, remap_send=remap_send, remap_target=remap_target, remap_counts=remap_counts, remap_weights=remap_weights, coupling=coupling, tracer=tracer, wet=wet, mix_inverse=mix_inverse, halo_send=halo_send, halo_ghost=halo_ghost, halo_rows=halo_rows)


def reference(atm_flux, remap_send, remap_target, remap_counts, remap_weights, coupling, tracer, wet, mix_inverse, halo_send, halo_ghost, halo_rows):
    wetf = wet.astype(jnp.float32)
    offsets = jnp.arange(SPAN, dtype=jnp.int32) - REACH
    blocks = atm_flux.reshape(F, N_PATCH * ABLK, BLOCK)

    def receive(ocean):
        source = (ocean - offsets) % N_PATCH
        global_id = source[:, None] * ABLK + remap_send[source, jnp.arange(SPAN, dtype=jnp.int32)]
        pieces = blocks[:, global_id].astype(jnp.float32)
        in_use = (jnp.arange(CAP, dtype=jnp.int32)[None, :] < remap_counts[ocean][:, None]).astype(jnp.float32)
        contrib = jnp.einsum("fdci,dcij->dcfj", pieces, remap_weights[ocean].astype(jnp.float32), precision=lax.Precision.HIGHEST)
        contrib = contrib * in_use[:, :, None, None]
        table = (remap_target[ocean][..., None] == jnp.arange(OBLK, dtype=jnp.int32)).astype(jnp.float32)
        return jnp.einsum("dcb,dcfj->fbj", table, contrib, precision=lax.Precision.HIGHEST).reshape(F, OBLK * BLOCK)

    flux = lax.map(receive, jnp.arange(N_PATCH, dtype=jnp.int32))
    ocean_flux = jnp.transpose(flux, (1, 0, 2)).reshape(F, NOC) * wetf
    surface = jnp.dot(coupling, ocean_flux, precision=lax.Precision.HIGHEST)
    rhs = tracer.at[:, 0, :].add(surface)
    shaped = rhs.reshape(NTR, LEV, N_PATCH * OBLK, BLOCK)
    solved = jnp.einsum("blk,tkbc->tlbc", mix_inverse, shaped, precision=lax.Precision.HIGHEST).reshape(NTR, LEV, NOC)
    mixed = wetf * solved + (1.0 - wetf) * tracer
    sent = mixed.astype(jnp.bfloat16)
    halo_offsets = jnp.concatenate([jnp.arange(-REACH, 0, dtype=jnp.int32), jnp.arange(1, REACH + 1, dtype=jnp.int32)])
    ocean_ids = jnp.arange(N_PATCH, dtype=jnp.int32)[:, None]
    source = (ocean_ids - halo_offsets[None, :]) % N_PATCH
    source_cells = halo_send[source, jnp.arange(HSPAN, dtype=jnp.int32)[None, :]]
    source_glob = source[:, :, None, None] * OC + source_cells
    target_glob = ocean_ids[:, :, None, None] * OC + halo_ghost
    in_use = (jnp.arange(HR, dtype=jnp.int32)[None, None, :] < halo_rows[:, :, None]).astype(jnp.float32)
    values = sent[:, :, source_glob].astype(jnp.float32)
    current = mixed[:, :, target_glob]
    weight = in_use[..., None] * wetf[target_glob]
    increment = 0.25 * (values - current) * weight
    tracer_out = mixed.at[:, :, target_glob].add(increment)
    return ocean_flux, tracer_out
```

```python
import functools

import jax
import jax.numpy as jnp
from jax import lax
from jax.experimental import pallas as pl
from jax.experimental.pallas import tpu as pltpu
from jax.sharding import PartitionSpec as P

F32 = jnp.float32
BF16 = jnp.bfloat16


def shifted(array, axis, by):
    length = lax.axis_size(axis)
    return lax.ppermute(array, axis, [(i, (i + by) % length) for i in range(length)])


def select_kernel(send_ref, atm_ref, *out_refs):
    offsets, capacity = send_ref.shape[1], send_ref.shape[2]
    cells = out_refs[0].shape[-1]
    for d in range(offsets):
        for c in range(capacity):
            start = pl.multiple_of(send_ref[0, d, c] * cells, cells)
            out_refs[d][c] = atm_ref[:, pl.ds(start, cells)]


def select_blocks(remap_send, atm_flux, cells):
    offsets, capacity = remap_send.shape[1], remap_send.shape[2]
    fluxes = atm_flux.shape[0]
    return pl.pallas_call(
        select_kernel,
        out_shape=[jax.ShapeDtypeStruct((capacity, fluxes, cells), BF16)] * offsets,
        in_specs=[
            pl.BlockSpec(memory_space=pltpu.SMEM),
            pl.BlockSpec(memory_space=pltpu.VMEM),
        ],
        out_specs=[pl.BlockSpec(memory_space=pltpu.VMEM)] * offsets,
        name="select_blocks",
    )(remap_send, atm_flux)


def split(x):
    high = x.astype(BF16)
    low = (x - high.astype(F32)).astype(BF16)
    return high, low


def lane_onehot(index_rows, cells):
    parts = []
    for q in range(index_rows.shape[0]):
        lane = index_rows[q : q + 1, :] & (cells - 1)
        sub = lax.broadcasted_iota(jnp.int32, (cells, index_rows.shape[1]), 0)
        parts.append(jnp.where(sub == lane, 1.0, 0.0).astype(BF16))
    return jnp.concatenate(parts, axis=1)


def mix_kernel(
    target_ref, count_ref, coupling_ref, *rest, offsets, capacity, group
):
    pieces = rest[:offsets]
    (wet_ref, send_ref, weights_hbm, tracer_hbm, inverse_hbm) = rest[offsets : offsets + 5]
    outs = rest[offsets + 5 :]
    flux_out = outs[0]
    mixed_hbm = outs[1]
    halo_count = offsets - 1
    halo_outs = outs[2 : 2 + halo_count]
    (
        weights, tracer, inverse, mixed, sent, acc, onehot, base,
        weight_sem, in_sems, out_sems,
    ) = outs[2 + halo_count :]
    tracers, levels, ocean_cells = tracer.shape
    cells = weights.shape[-1]
    blocks = ocean_cells // cells
    groups = blocks // group
    span = group * cells
    fluxes = flux_out.shape[0]

    def load(g):
        lanes = pl.ds(g * span, span)
        return (
            pltpu.make_async_copy(
                tracer_hbm.at[:, :, lanes], tracer.at[:, :, lanes], in_sems.at[0, g]
            ),
            pltpu.make_async_copy(
                inverse_hbm.at[pl.ds(g * group, group)],
                inverse.at[pl.ds(g * group, group)],
                in_sems.at[1, g],
            ),
        )

    def store(g):
        lanes = pl.ds(g * span, span)
        return pltpu.make_async_copy(
            mixed.at[:, :, lanes], mixed_hbm.at[:, :, lanes], out_sems.at[g]
        )

    weight_copy = pltpu.make_async_copy(weights_hbm, weights, weight_sem)
    weight_copy.start()
    for g in range(groups):
        for copy in load(g):
            copy.start()

    base[...] = lane_onehot(send_ref[...], cells)
    block_row = jnp.concatenate(
        [send_ref[q : q + 1, :] // cells for q in range(send_ref.shape[0])], axis=1
    )

    acc[...] = jnp.zeros_like(acc)
    weight_copy.wait()
    for d in range(offsets):
        for c in range(capacity):
            contrib = jnp.dot(
                pieces[d][c], weights[d * capacity + c], preferred_element_type=F32
            )
            used = jnp.where(c < count_ref[0, d], 1.0, 0.0).astype(F32)
            start = pl.multiple_of(target_ref[0, d, c] * cells, cells)
            acc[:, pl.ds(start, cells)] += contrib * used

    sub = lax.broadcasted_iota(jnp.int32, (fluxes, cells), 0)
    couple = []
    for t in range(tracers):
        col = jnp.zeros((fluxes, cells), F32)
        for f in range(fluxes):
            col = jnp.where(sub == f, coupling_ref[t, f], col)
        couple.append(col)
    top = lax.broadcasted_iota(jnp.int32, (levels, cells), 0) == 0

    for g in range(groups):
        for copy in load(g):
            copy.wait()
        for i in range(group):
            b = g * group + i
            lanes = slice(b * cells, (b + 1) * cells)
            wet = wet_ref[b : b + 1, :].astype(F32)
            flux = acc[:, lanes] * wet
            flux_out[:, lanes] = flux
            highs, lows, raw = [], [], []
            for t in range(tracers):
                surface = jnp.sum(couple[t] * flux, axis=0, keepdims=True)
                value = tracer[t, :, lanes]
                raw.append(value)
                high, low = split(value + jnp.where(top, surface, 0.0))
                highs.append(high)
                lows.append(low)
            high = jnp.concatenate(highs, axis=1)
            low = jnp.concatenate(lows, axis=1)
            m_high, m_low = split(inverse[b])
            left = jnp.concatenate([m_high, m_low], axis=1)
            right = jnp.concatenate([high, high], axis=0)
            solved = jnp.dot(left, right, preferred_element_type=F32) + jnp.dot(
                m_high, low, preferred_element_type=F32
            )
            for t in range(tracers):
                value = jnp.where(
                    wet > 0.5, solved[:, t * cells : (t + 1) * cells], raw[t]
                )
                mixed[t, :, lanes] = value
                sent[t * levels : (t + 1) * levels, lanes] = value.astype(BF16)
            onehot[lanes, :] = base[...] * jnp.where(block_row == b, 1.0, 0.0).astype(BF16)
        store(g).start()

    picks = onehot.shape[1] // halo_count
    for h in range(halo_count):
        halo_outs[h][...] = jnp.dot(
            sent[...], onehot[:, h * picks : (h + 1) * picks], preferred_element_type=F32
        ).astype(BF16)
    for g in range(groups):
        store(g).wait()


def mix(pieces, remap_target, remap_counts, remap_weights, coupling, tracer, wet, mix_inverse, halo_send):
    offsets, capacity = remap_target.shape[1:]
    tracers, levels, ocean_cells = tracer.shape
    cells = remap_weights.shape[-1]
    blocks = ocean_cells // cells
    fluxes = pieces[0].shape[1]
    halo_count, depth, lanes = halo_send.shape[1:]
    picks = depth * lanes
    group = 4 if blocks % 4 == 0 else 1
    groups = blocks // group
    smem = pl.BlockSpec(memory_space=pltpu.SMEM)
    vmem = pl.BlockSpec(memory_space=pltpu.VMEM)
    hbm = pl.BlockSpec(memory_space=pl.ANY)
    return pl.pallas_call(
        functools.partial(mix_kernel, offsets=offsets, capacity=capacity, group=group),
        out_shape=[
            jax.ShapeDtypeStruct((fluxes, ocean_cells), F32),
            jax.ShapeDtypeStruct(tracer.shape, F32),
        ]
        + [jax.ShapeDtypeStruct((tracers * levels, picks), BF16)] * halo_count,
        in_specs=[smem, smem, smem] + [vmem] * offsets + [vmem, vmem, hbm, hbm, hbm],
        out_specs=[vmem, hbm] + [vmem] * halo_count,
        scratch_shapes=[
            pltpu.VMEM((offsets * capacity, cells, cells), BF16),
            pltpu.VMEM(tracer.shape, F32),
            pltpu.VMEM((blocks, levels, levels), F32),
            pltpu.VMEM(tracer.shape, F32),
            pltpu.VMEM((tracers * levels, ocean_cells), BF16),
            pltpu.VMEM((fluxes, ocean_cells), F32),
            pltpu.VMEM((ocean_cells, halo_count * picks), BF16),
            pltpu.VMEM((cells, halo_count * picks), BF16),
            pltpu.SemaphoreType.DMA,
            pltpu.SemaphoreType.DMA((2, groups)),
            pltpu.SemaphoreType.DMA((groups,)),
        ],
        name="mix",
    )(
        remap_target,
        remap_counts,
        coupling,
        *pieces,
        wet.reshape(blocks, cells),
        halo_send.reshape(halo_count * depth, lanes),
        remap_weights.reshape(offsets * capacity, cells, cells),
        tracer,
        mix_inverse,
    )


def apply_kernel(rows_ref, ghost_ref, wet_ref, *rest, halo_count, depth):
    values = rest[:halo_count]
    mixed_ref, out_ref, base, left = rest[halo_count:]
    tracers, levels, span = mixed_ref.shape
    cells = wet_ref.shape[1]
    group = span // cells
    step = pl.program_id(0)
    rows = tracers * levels
    picks = values[0].shape[1]

    @pl.when(step == 0)
    def _():
        base[...] = lane_onehot(ghost_ref[...], cells)
        for h in range(halo_count):
            left[0:rows, h * picks : (h + 1) * picks] = values[h][...]
        left[rows:, :] = jnp.ones((left.shape[0] - rows, left.shape[1]), BF16)

    block_row = []
    for h in range(halo_count):
        for r in range(depth):
            q = h * depth + r
            block = ghost_ref[q : q + 1, :] // cells
            block_row.append(jnp.where(r < rows_ref[0, h], block, -1))
    block_row = jnp.concatenate(block_row, axis=1)
    onehots = []
    for i in range(group):
        b = step * group + i
        onehots.append(base[...] * jnp.where(block_row == b, 1.0, 0.0).astype(BF16))
    onehot = jnp.concatenate(onehots, axis=0)
    total = lax.dot_general(
        left[...], onehot, (((1,), (1,)), ((), ())), preferred_element_type=F32
    )
    count = total[rows : rows + 1, :]
    for i in range(group):
        b = step * group + i
        lanes = slice(i * cells, (i + 1) * cells)
        quarter = 0.25 * wet_ref[pl.ds(b, 1), :].astype(F32)
        keep = 1.0 - quarter * count[:, lanes]
        for t in range(tracers):
            out_ref[t, :, lanes] = (
                mixed_ref[t, :, lanes] * keep
                + total[t * levels : (t + 1) * levels, lanes] * quarter
            )


def apply_halo(values, mixed, wet, halo_ghost, halo_rows):
    tracers, levels, ocean_cells = mixed.shape
    halo_count, depth, lanes = halo_ghost.shape[1:]
    cells = lanes
    blocks = ocean_cells // cells
    picks = halo_count * depth * lanes
    group = 4 if blocks % 4 == 0 else 1
    span = group * cells
    smem = pl.BlockSpec(memory_space=pltpu.SMEM)
    vmem = pl.BlockSpec(memory_space=pltpu.VMEM)
    block = pl.BlockSpec((tracers, levels, span), lambda g: (0, 0, g))
    return pl.pallas_call(
        functools.partial(apply_kernel, halo_count=halo_count, depth=depth),
        grid=(blocks // group,),
        out_shape=jax.ShapeDtypeStruct(mixed.shape, F32),
        in_specs=[smem, vmem, vmem] + [vmem] * halo_count + [block],
        out_specs=block,
        scratch_shapes=[
            pltpu.VMEM((cells, picks), BF16),
            pltpu.VMEM((tracers * levels + 16, picks), BF16),
        ],
        name="apply_halo",
    )(
        halo_rows,
        halo_ghost.reshape(halo_count * depth, lanes),
        wet.reshape(blocks, cells),
        *values,
        mixed,
    )


def body(
    atm_flux,
    remap_send,
    remap_target,
    remap_counts,
    remap_weights,
    coupling,
    tracer,
    wet,
    mix_inverse,
    halo_send,
    halo_ghost,
    halo_rows,
):
    offsets = remap_send.shape[1]
    radius = offsets // 2
    cells = remap_weights.shape[-1]
    outgoing = select_blocks(remap_send, atm_flux, cells)
    pieces = [
        outgoing[d] if d == radius else shifted(outgoing[d], "patch", d - radius)
        for d in range(offsets)
    ]
    ocean_flux, mixed, *halo_out = mix(
        pieces, remap_target, remap_counts, remap_weights[0], coupling, tracer, wet,
        mix_inverse, halo_send,
    )
    halo_offsets = [e for e in range(-radius, radius + 1) if e]
    values = [shifted(halo_out[h], "patch", halo_offsets[h]) for h in range(len(halo_out))]
    return ocean_flux, apply_halo(values, mixed, wet, halo_ghost, halo_rows)


def solution(mesh):
    return jax.shard_map(
        body,
        mesh=mesh,
        in_specs=(
            P(None, "patch"),
            P("patch", None, None),
            P("patch", None, None),
            P("patch", None),
            P("patch", None, None, None, None),
            P(),
            P(None, None, "patch"),
            P("patch"),
            P("patch", None, None),
            P("patch", None, None, None),
            P("patch", None, None, None),
            P("patch", None),
        ),
        out_specs=(P(None, "patch"), P(None, None, "patch")),
        check_vma=False,
    )
```

```python
import functools

import jax
import jax.numpy as jnp
from jax import lax
from jax.experimental import pallas as pl
from jax.experimental.pallas import tpu as pltpu
from jax.sharding import PartitionSpec as P

F32 = jnp.float32
BF16 = jnp.bfloat16


def shifted(array, axis, by):
    length = lax.axis_size(axis)
    return lax.ppermute(array, axis, [(i, (i + by) % length) for i in range(length)])


def vmem_out(shape, dtype):
    return pltpu.VMEM(shape, dtype)


def pinned(*arrays):
    return [pltpu.with_memory_space_constraint(a, pltpu.VMEM) for a in arrays]


def in_hbm(*arrays):
    return [pltpu.with_memory_space_constraint(a, pltpu.HBM) for a in arrays]


SMEM_SPEC = pl.BlockSpec(memory_space=pltpu.SMEM)
VMEM_SPEC = pl.BlockSpec(memory_space=pltpu.VMEM)
ANY_SPEC = pl.BlockSpec(memory_space=pl.ANY)
PARAMS = pltpu.CompilerParams(vmem_limit_bytes=16 * 2**20)


def select_kernel(send_ref, atm_ref, *out_refs):
    offsets, capacity = send_ref.shape[0], send_ref.shape[2]
    cells = out_refs[0].shape[-1]
    for d in range(offsets):
        for c in range(capacity):
            start = pl.multiple_of(send_ref[d, 0, c] * cells, cells)
            out_refs[d][c] = atm_ref[:, pl.ds(start, cells)]


def select_blocks(remap_send, atm_flux, cells):
    offsets, capacity = remap_send.shape[1], remap_send.shape[2]
    fluxes = atm_flux.shape[0]
    return pl.pallas_call(
        select_kernel,
        out_shape=[vmem_out((capacity, fluxes, cells), BF16)] * offsets,
        in_specs=[SMEM_SPEC, VMEM_SPEC],
        out_specs=[VMEM_SPEC] * offsets,
        compiler_params=PARAMS,
        name="select_blocks",
    )(*in_hbm(jnp.transpose(remap_send, (1, 0, 2)), atm_flux))


def split(x):
    high = x.astype(BF16)
    low = (x - high.astype(F32)).astype(BF16)
    return high, low


def lane_onehot(index_ref, cells):
    parts = []
    sub = lax.broadcasted_iota(jnp.int32, (cells, index_ref.shape[1]), 0)
    for q in range(index_ref.shape[0]):
        lane = index_ref[q : q + 1, :] & (cells - 1)
        parts.append(jnp.where(sub == lane, 1.0, 0.0).astype(BF16))
    return jnp.concatenate(parts, axis=1)


def block_mask(block_row, b):
    return jnp.where(block_row == b, 1.0, 0.0).astype(BF16)


def premix_kernel(
    wet_hbm, send_hbm, tracer_hbm, inverse_hbm, mixed, column, onehot, wetf,
    wet_ref, send_ref, base, tracer, inverse, small_sems, sems, *, group
):
    tracers, levels, ocean_cells = tracer.shape
    blocks, cells = wet_ref.shape
    small = (
        pltpu.make_async_copy(wet_hbm, wet_ref, small_sems.at[0]),
        pltpu.make_async_copy(send_hbm, send_ref, small_sems.at[1]),
    )
    for copy in small:
        copy.start()

    def load(g):
        lanes = pl.ds(g * group * cells, group * cells)
        rows = pl.ds(g * group, group)
        return (
            pltpu.make_async_copy(
                tracer_hbm.at[:, :, lanes], tracer.at[:, :, lanes], sems.at[0, g]
            ),
            pltpu.make_async_copy(inverse_hbm.at[rows], inverse.at[rows], sems.at[1, g]),
        )

    for g in range(blocks // group):
        for copy in load(g):
            copy.start()
    for copy in small:
        copy.wait()
    wetf[...] = wet_ref[...].astype(F32)
    base[...] = lane_onehot(send_ref, cells)
    block_row = jnp.concatenate(
        [send_ref[q : q + 1, :] // cells for q in range(send_ref.shape[0])], axis=1
    )
    for b in range(blocks):
        if b % group == 0:
            for copy in load(b // group):
                copy.wait()
        lanes = slice(b * cells, (b + 1) * cells)
        wet = wetf[b : b + 1, :]
        highs, lows, raw = [], [], []
        for t in range(tracers):
            value = tracer[t, :, lanes]
            raw.append(value)
            high, low = split(value)
            highs.append(high)
            lows.append(low)
        high = jnp.concatenate(highs, axis=1)
        low = jnp.concatenate(lows, axis=1)
        matrix = inverse[b]
        m_high, m_low = split(matrix)
        left = jnp.concatenate([m_high, m_low], axis=1)
        right = jnp.concatenate([high, high], axis=0)
        solved = jnp.dot(left, right, preferred_element_type=F32) + jnp.dot(
            m_high, low, preferred_element_type=F32
        )
        for t in range(tracers):
            mixed[t, :, lanes] = jnp.where(
                wet > 0.5, solved[:, t * cells : (t + 1) * cells], raw[t]
            )
        column[b] = jnp.broadcast_to(matrix[:, 0:1], (levels, cells))
        onehot[lanes, :] = base[...] * block_mask(block_row, b)


def premix(tracer, wet, mix_inverse, halo_send):
    tracers, levels, ocean_cells = tracer.shape
    blocks = mix_inverse.shape[0]
    cells = ocean_cells // blocks
    halo_count, depth, lanes = halo_send.shape[1:]
    picks = halo_count * depth * lanes
    group = 4 if blocks % 4 == 0 else 1
    return pl.pallas_call(
        functools.partial(premix_kernel, group=group),
        out_shape=[
            vmem_out(tracer.shape, F32),
            vmem_out((blocks, levels, cells), F32),
            vmem_out((ocean_cells, picks), BF16),
            vmem_out((blocks, cells), F32),
        ],
        in_specs=[ANY_SPEC] * 4,
        out_specs=[VMEM_SPEC] * 4,
        scratch_shapes=[
            pltpu.VMEM((blocks, cells), jnp.int32),
            pltpu.VMEM((halo_count * depth, lanes), jnp.int32),
            pltpu.VMEM((cells, picks), BF16),
            pltpu.VMEM(tracer.shape, F32),
            pltpu.VMEM(mix_inverse.shape, F32),
            pltpu.SemaphoreType.DMA((2,)),
            pltpu.SemaphoreType.DMA((2, blocks // group)),
        ],
        compiler_params=PARAMS,
        name="premix",
    )(
        *in_hbm(
            wet.reshape(blocks, cells),
            halo_send.reshape(halo_count * depth, lanes),
            tracer,
            mix_inverse,
        )
    )


def finish_kernel(target_ref, count_ref, coupling_ref, *rest, offsets, capacity):
    pieces = rest[:offsets]
    wet_ref, weights, mixed0, column, onehot = rest[offsets : offsets + 5]
    outs = rest[offsets + 5 :]
    flux_out, mixed = outs[:2]
    halo_count = offsets - 1
    halo_outs = outs[2 : 2 + halo_count]
    sent, acc = outs[2 + halo_count :]
    tracers, levels, ocean_cells = mixed0.shape
    blocks, cells = wet_ref.shape
    fluxes = flux_out.shape[0]

    acc[...] = jnp.zeros_like(acc)
    for d in range(offsets):
        for c in range(capacity):
            contrib = jnp.dot(
                pieces[d][c], weights[d * capacity + c], preferred_element_type=F32
            )
            used = jnp.where(c < count_ref[0, d], 1.0, 0.0).astype(F32)
            start = pl.multiple_of(target_ref[d, 0, c] * cells, cells)
            acc[:, pl.ds(start, cells)] += contrib * used

    sub = lax.broadcasted_iota(jnp.int32, (fluxes, cells), 0)
    couple = []
    for t in range(tracers):
        col = jnp.zeros((fluxes, cells), F32)
        for f in range(fluxes):
            col = jnp.where(sub == f, coupling_ref[t, f], col)
        couple.append(col)

    for b in range(blocks):
        lanes = slice(b * cells, (b + 1) * cells)
        flux = acc[:, lanes] * wet_ref[b : b + 1, :]
        flux_out[:, lanes] = flux
        for t in range(tracers):
            surface = jnp.sum(couple[t] * flux, axis=0, keepdims=True)
            value = mixed0[t, :, lanes] + column[b] * surface
            mixed[t, :, lanes] = value
            sent[t * levels : (t + 1) * levels, lanes] = value.astype(BF16)

    picks = onehot.shape[1] // halo_count
    for h in range(halo_count):
        halo_outs[h][...] = jnp.dot(
            sent[...], onehot[:, h * picks : (h + 1) * picks], preferred_element_type=F32
        ).astype(BF16)


def finish(pieces, remap_target, remap_counts, remap_weights, coupling, wetf, mixed0, column, onehot):
    offsets, capacity = remap_target.shape[1:]
    tracers, levels, ocean_cells = mixed0.shape
    cells = remap_weights.shape[-1]
    blocks = ocean_cells // cells
    fluxes = pieces[0].shape[1]
    halo_count = offsets - 1
    picks = onehot.shape[1] // halo_count
    return pl.pallas_call(
        functools.partial(finish_kernel, offsets=offsets, capacity=capacity),
        out_shape=[
            jax.ShapeDtypeStruct((fluxes, ocean_cells), F32),
            vmem_out(mixed0.shape, F32),
        ]
        + [vmem_out((tracers * levels, picks), BF16)] * halo_count,
        in_specs=[SMEM_SPEC] * 3 + [VMEM_SPEC] * (offsets + 5),
        out_specs=[VMEM_SPEC] * (2 + halo_count),
        scratch_shapes=[
            pltpu.VMEM((tracers * levels, ocean_cells), BF16),
            pltpu.VMEM((fluxes, ocean_cells), F32),
        ],
        input_output_aliases={3 + offsets + 2: 1},
        compiler_params=PARAMS,
        name="finish",
    )(
        jnp.transpose(remap_target, (1, 0, 2)),
        remap_counts,
        coupling,
        *pinned(*pieces, wetf),
        *pinned(remap_weights.reshape(offsets * capacity, cells, cells)),
        *pinned(mixed0, column, onehot),
    )


def preapply_kernel(rows_ref, ghost_ref, wet_ref, mixed, kept, onehot, base, *, halo_count, depth):
    tracers, levels, ocean_cells = mixed.shape
    blocks, cells = wet_ref.shape
    picks = onehot.shape[1]
    base[...] = lane_onehot(ghost_ref, cells)
    block_row = []
    for h in range(halo_count):
        for r in range(depth):
            q = h * depth + r
            block = ghost_ref[q : q + 1, :] // cells
            block_row.append(jnp.where(r < rows_ref[0, h], block, -1))
    block_row = jnp.concatenate(block_row, axis=1)
    ones = jnp.ones((16, picks), BF16)
    for b in range(blocks):
        lanes = slice(b * cells, (b + 1) * cells)
        hot = base[...] * block_mask(block_row, b)
        onehot[lanes, :] = hot
        count = lax.dot_general(
            ones, hot, (((1,), (1,)), ((), ())), preferred_element_type=F32
        )[0:1, :]
        keep = 1.0 - 0.25 * wet_ref[b : b + 1, :] * count
        for t in range(tracers):
            kept[t, :, lanes] = mixed[t, :, lanes] * keep


def preapply(mixed, wetf, halo_ghost, halo_rows):
    tracers, levels, ocean_cells = mixed.shape
    halo_count, depth, lanes = halo_ghost.shape[1:]
    cells = lanes
    blocks = ocean_cells // cells
    picks = halo_count * depth * lanes
    return pl.pallas_call(
        functools.partial(preapply_kernel, halo_count=halo_count, depth=depth),
        out_shape=[vmem_out(mixed.shape, F32), vmem_out((ocean_cells, picks), BF16)],
        in_specs=[SMEM_SPEC] + [VMEM_SPEC] * 3,
        out_specs=[VMEM_SPEC] * 2,
        scratch_shapes=[pltpu.VMEM((cells, picks), BF16)],
        input_output_aliases={3: 0},
        compiler_params=PARAMS,
        name="preapply",
    )(
        halo_rows,
        halo_ghost.reshape(halo_count * depth, lanes),
        *pinned(wetf, mixed),
    )


def apply_kernel(wet_ref, *rest, halo_count, group):
    values = rest[:halo_count]
    kept, onehot, out_hbm, staged, sems = rest[halo_count:]
    tracers, levels, ocean_cells = kept.shape
    blocks, cells = wet_ref.shape
    span = group * cells
    picks = values[0].shape[1]

    def store(g):
        lanes = pl.ds(g * span, span)
        return pltpu.make_async_copy(
            staged.at[:, :, lanes], out_hbm.at[:, :, lanes], sems.at[g]
        )

    left = jnp.concatenate([v[...] for v in values], axis=1)
    for g in range(blocks // group):
        total = lax.dot_general(
            left,
            onehot[g * span : (g + 1) * span, :],
            (((1,), (1,)), ((), ())),
            preferred_element_type=F32,
        )
        for i in range(group):
            b = g * group + i
            lanes = slice(b * cells, (b + 1) * cells)
            here = slice(i * cells, (i + 1) * cells)
            quarter = 0.25 * wet_ref[b : b + 1, :]
            for t in range(tracers):
                staged[t, :, lanes] = (
                    kept[t, :, lanes] + total[t * levels : (t + 1) * levels, here] * quarter
                )
        store(g).start()
    for g in range(blocks // group):
        store(g).wait()


def apply_halo(values, kept, onehot, wetf):
    tracers, levels, ocean_cells = kept.shape
    halo_count = len(values)
    picks = onehot.shape[1] // halo_count
    cells = wetf.shape[1]
    blocks = ocean_cells // cells
    group = 4 if blocks % 4 == 0 else 1
    return pl.pallas_call(
        functools.partial(apply_kernel, halo_count=halo_count, group=group),
        out_shape=jax.ShapeDtypeStruct(kept.shape, F32),
        in_specs=[VMEM_SPEC] * (halo_count + 3),
        out_specs=ANY_SPEC,
        scratch_shapes=[
            pltpu.VMEM(kept.shape, F32),
            pltpu.SemaphoreType.DMA((blocks // group,)),
        ],
        compiler_params=PARAMS,
        name="apply_halo",
    )(*pinned(wetf, *values, kept, onehot))


def body(
    atm_flux,
    remap_send,
    remap_target,
    remap_counts,
    remap_weights,
    coupling,
    tracer,
    wet,
    mix_inverse,
    halo_send,
    halo_ghost,
    halo_rows,
):
    offsets = remap_send.shape[1]
    radius = offsets // 2
    cells = remap_weights.shape[-1]
    outgoing = select_blocks(remap_send, atm_flux, cells)
    pieces = [
        outgoing[d] if d == radius else shifted(outgoing[d], "patch", d - radius)
        for d in range(offsets)
    ]
    mixed0, column, onehot, wetf = premix(tracer, wet, mix_inverse, halo_send)
    ocean_flux, mixed, *halo_out = finish(
        pieces, remap_target, remap_counts, remap_weights[0], coupling, wetf, mixed0, column, onehot
    )
    halo_offsets = [e for e in range(-radius, radius + 1) if e]
    values = [shifted(halo_out[h], "patch", halo_offsets[h]) for h in range(len(halo_out))]
    kept, ghosts = preapply(mixed, wetf, halo_ghost, halo_rows)
    return ocean_flux, apply_halo(values, kept, ghosts, wetf)


def solution(mesh):
    return jax.shard_map(
        body,
        mesh=mesh,
        in_specs=(
            P(None, "patch"),
            P("patch", None, None),
            P("patch", None, None),
            P("patch", None),
            P("patch", None, None, None, None),
            P(),
            P(None, None, "patch"),
            P("patch"),
            P("patch", None, None),
            P("patch", None, None, None),
            P("patch", None, None, None),
            P("patch", None),
        ),
        out_specs=(P(None, "patch"), P(None, None, "patch")),
        check_vma=False,
    )
```

```python
import functools

import jax
import jax.numpy as jnp
from jax import lax
from jax.experimental import pallas as pl
from jax.experimental.pallas import tpu as pltpu
from jax.sharding import PartitionSpec as P

F32 = jnp.float32
BF16 = jnp.bfloat16


def shifted(array, axis, by):
    length = lax.axis_size(axis)
    return lax.ppermute(array, axis, [(i, (i + by) % length) for i in range(length)])


def flux_order(radius):
    return [e for e in range(-radius, radius + 1) if e]


def halo_order(radius):
    return list(range(radius, 0, -1)) + list(range(-radius, 0))


def vmem_out(shape, dtype):
    return pltpu.VMEM(shape, dtype)


def pinned(*arrays):
    return [pltpu.with_memory_space_constraint(a, pltpu.VMEM) for a in arrays]


def in_hbm(*arrays):
    return [pltpu.with_memory_space_constraint(a, pltpu.HBM) for a in arrays]


SMEM_SPEC = pl.BlockSpec(memory_space=pltpu.SMEM)
VMEM_SPEC = pl.BlockSpec(memory_space=pltpu.VMEM)
ANY_SPEC = pl.BlockSpec(memory_space=pl.ANY)
PARAMS = pltpu.CompilerParams(vmem_limit_bytes=16 * 2**20)


def select_kernel(send_ref, atm_ref, *out_refs):
    offsets, capacity = send_ref.shape[0], send_ref.shape[2]
    cells = out_refs[0].shape[-1]
    for d in range(offsets):
        for c in range(capacity):
            start = pl.multiple_of(send_ref[d, 0, c] * cells, cells)
            out_refs[d][c] = atm_ref[:, pl.ds(start, cells)]


def select_blocks(remap_send, atm_flux, cells):
    offsets, capacity = remap_send.shape[1], remap_send.shape[2]
    fluxes = atm_flux.shape[0]
    return pl.pallas_call(
        select_kernel,
        out_shape=[vmem_out((capacity, fluxes, cells), BF16)] * offsets,
        in_specs=[SMEM_SPEC, VMEM_SPEC],
        out_specs=[VMEM_SPEC] * offsets,
        compiler_params=PARAMS,
        name="select_blocks",
    )(*in_hbm(jnp.transpose(remap_send, (1, 0, 2)), atm_flux))


def split(x):
    high = x.astype(BF16)
    low = (x - high.astype(F32)).astype(BF16)
    return high, low


def lane_onehot(index_ref, cells):
    parts = []
    sub = lax.broadcasted_iota(jnp.int32, (cells, index_ref.shape[1]), 0)
    for q in range(index_ref.shape[0]):
        lane = index_ref[q : q + 1, :] & (cells - 1)
        parts.append(jnp.where(sub == lane, 1.0, 0.0).astype(BF16))
    return jnp.concatenate(parts, axis=1)


def block_mask(block_row, b):
    return jnp.where(block_row == b, 1.0, 0.0).astype(BF16)


def premix_kernel(
    wet_hbm, send_hbm, tracer_hbm, inverse_hbm, mixed, column, onehot, wetf,
    wet_ref, send_ref, base, tracer, inverse, small_sems, sems, *, cuts
):
    tracers, levels, ocean_cells = tracer.shape
    blocks, cells = wet_ref.shape
    small = (
        pltpu.make_async_copy(wet_hbm, wet_ref, small_sems.at[0]),
        pltpu.make_async_copy(send_hbm, send_ref, small_sems.at[1]),
    )
    for copy in small:
        copy.start()

    def load(g):
        first, size = cuts[g], cuts[g + 1] - cuts[g]
        lanes = pl.ds(first * cells, size * cells)
        rows = pl.ds(first, size)
        return (
            pltpu.make_async_copy(
                tracer_hbm.at[:, :, lanes], tracer.at[:, :, lanes], sems.at[0, g]
            ),
            pltpu.make_async_copy(inverse_hbm.at[rows], inverse.at[rows], sems.at[1, g]),
        )

    for g in range(len(cuts) - 1):
        for copy in load(g):
            copy.start()
    for copy in small:
        copy.wait()
    wetf[...] = wet_ref[...].astype(F32)
    base[...] = lane_onehot(send_ref, cells)
    block_row = jnp.concatenate(
        [send_ref[q : q + 1, :] // cells for q in range(send_ref.shape[0])], axis=1
    )
    for b in range(blocks):
        if b in cuts:
            for copy in load(cuts.index(b)):
                copy.wait()
        lanes = slice(b * cells, (b + 1) * cells)
        wet = wetf[b : b + 1, :]
        highs, lows, raw = [], [], []
        for t in range(tracers):
            value = tracer[t, :, lanes]
            raw.append(value)
            high, low = split(value)
            highs.append(high)
            lows.append(low)
        high = jnp.concatenate(highs, axis=1)
        low = jnp.concatenate(lows, axis=1)
        matrix = inverse[b]
        m_high, m_low = split(matrix)
        left = jnp.concatenate([m_high, m_low], axis=1)
        right = jnp.concatenate([high, high], axis=0)
        solved = jnp.dot(left, right, preferred_element_type=F32) + jnp.dot(
            m_high, low, preferred_element_type=F32
        )
        for t in range(tracers):
            mixed[t, :, lanes] = jnp.where(
                wet > 0.5, solved[:, t * cells : (t + 1) * cells], raw[t]
            )
        column[b] = jnp.broadcast_to(matrix[:, 0:1], (levels, cells))
        onehot[lanes, :] = base[...] * block_mask(block_row, b)


def premix(tracer, wet, mix_inverse, halo_send):
    tracers, levels, ocean_cells = tracer.shape
    blocks = mix_inverse.shape[0]
    cells = ocean_cells // blocks
    halo_count, depth, lanes = halo_send.shape[1:]
    picks = halo_count * depth * lanes
    cuts = (0, blocks // 4, blocks)
    return pl.pallas_call(
        functools.partial(premix_kernel, cuts=cuts),
        out_shape=[
            vmem_out(tracer.shape, F32),
            vmem_out((blocks, levels, cells), F32),
            vmem_out((ocean_cells, picks), BF16),
            vmem_out((blocks, cells), F32),
        ],
        in_specs=[ANY_SPEC] * 4,
        out_specs=[VMEM_SPEC] * 4,
        scratch_shapes=[
            pltpu.VMEM((blocks, cells), jnp.int32),
            pltpu.VMEM((halo_count * depth, lanes), jnp.int32),
            pltpu.VMEM((cells, picks), BF16),
            pltpu.VMEM(tracer.shape, F32),
            pltpu.VMEM(mix_inverse.shape, F32),
            pltpu.SemaphoreType.DMA((2,)),
            pltpu.SemaphoreType.DMA((2, len(cuts) - 1)),
        ],
        compiler_params=PARAMS,
        name="premix",
    )(
        *in_hbm(
            wet.reshape(blocks, cells),
            halo_send.reshape(halo_count * depth, lanes),
            tracer,
            mix_inverse,
        )
    )


def finish_kernel(target_vmem, count_vmem, coupling_vmem, *rest, offsets, capacity):
    radius = offsets // 2
    order = flux_order(radius) + [0]
    pieces = [rest[order.index(e)] for e in range(-radius, radius + 1)]
    wet_ref, weights, mixed0, column, onehot = rest[offsets : offsets + 5]
    outs = rest[offsets + 5 :]
    flux_out, mixed = outs[:2]
    halo_count = offsets - 1
    halo_outs = outs[2 : 2 + halo_count]
    sent, acc, parts, target_ref, count_ref, coupling_ref, sems = outs[2 + halo_count :]
    tracers, levels, ocean_cells = mixed0.shape
    blocks, cells = wet_ref.shape
    fluxes = flux_out.shape[0]

    small = (
        pltpu.make_async_copy(target_vmem, target_ref, sems.at[0]),
        pltpu.make_async_copy(count_vmem, count_ref, sems.at[1]),
        pltpu.make_async_copy(coupling_vmem, coupling_ref, sems.at[2]),
    )
    for copy in small:
        copy.start()
    acc[...] = jnp.zeros_like(acc)
    for d in range(offsets):
        for c in range(capacity):
            parts[d * capacity + c] = jnp.dot(
                pieces[d][c], weights[d * capacity + c], preferred_element_type=F32
            )
    for copy in small:
        copy.wait()
    for d in range(offsets):
        for c in range(capacity):
            used = jnp.where(c < count_ref[0, d], 1.0, 0.0).astype(F32)
            start = pl.multiple_of(target_ref[d, 0, c] * cells, cells)
            acc[:, pl.ds(start, cells)] += parts[d * capacity + c] * used

    sub = lax.broadcasted_iota(jnp.int32, (fluxes, cells), 0)
    couple = []
    for t in range(tracers):
        col = jnp.zeros((fluxes, cells), F32)
        for f in range(fluxes):
            col = jnp.where(sub == f, coupling_ref[t, f], col)
        couple.append(col)

    for b in range(blocks):
        lanes = slice(b * cells, (b + 1) * cells)
        flux = acc[:, lanes] * wet_ref[b : b + 1, :]
        flux_out[:, lanes] = flux
        for t in range(tracers):
            surface = jnp.sum(couple[t] * flux, axis=0, keepdims=True)
            value = mixed0[t, :, lanes] + column[b] * surface
            mixed[t, :, lanes] = value
            sent[t * levels : (t + 1) * levels, lanes] = value.astype(BF16)

    picks = onehot.shape[1] // halo_count
    for h in range(halo_count):
        halo_outs[h][...] = jnp.dot(
            sent[...], onehot[:, h * picks : (h + 1) * picks], preferred_element_type=F32
        ).astype(BF16)


def finish(pieces, remap_target, remap_counts, remap_weights, coupling, wetf, mixed0, column, onehot):
    offsets, capacity = remap_target.shape[1:]
    tracers, levels, ocean_cells = mixed0.shape
    cells = remap_weights.shape[-1]
    blocks = ocean_cells // cells
    fluxes = pieces[0].shape[1]
    halo_count = offsets - 1
    picks = onehot.shape[1] // halo_count
    return pl.pallas_call(
        functools.partial(finish_kernel, offsets=offsets, capacity=capacity),
        out_shape=[
            vmem_out((fluxes, ocean_cells), F32),
            vmem_out(mixed0.shape, F32),
        ]
        + [vmem_out((tracers * levels, picks), BF16)] * halo_count,
        in_specs=[ANY_SPEC] * 3 + [VMEM_SPEC] * (offsets + 5),
        out_specs=[VMEM_SPEC] * (2 + halo_count),
        scratch_shapes=[
            pltpu.VMEM((tracers * levels, ocean_cells), BF16),
            pltpu.VMEM((fluxes, ocean_cells), F32),
            pltpu.VMEM((offsets * capacity, fluxes, cells), F32),
            pltpu.SMEM((offsets, 1, capacity), jnp.int32),
            pltpu.SMEM(remap_counts.shape, jnp.int32),
            pltpu.SMEM(coupling.shape, F32),
            pltpu.SemaphoreType.DMA((3,)),
        ],
        input_output_aliases={3 + offsets + 2: 1},
        compiler_params=PARAMS,
        name="finish",
    )(
        *pinned(jnp.transpose(remap_target, (1, 0, 2)), remap_counts, coupling),
        *pinned(*[pieces[e + offsets // 2] for e in flux_order(offsets // 2) + [0]], wetf),
        *pinned(remap_weights.reshape(offsets * capacity, cells, cells)),
        *pinned(mixed0, column, onehot),
    )


def ghost_kernel(
    rows_ref, ghost_ref, wetf, mixed_unused, onehot, keep, base, *, halo_count, depth
):
    blocks, cells = wetf.shape
    base[...] = lane_onehot(ghost_ref, cells)
    block_row = []
    for h in range(halo_count):
        for r in range(depth):
            q = h * depth + r
            block = ghost_ref[q : q + 1, :] // cells
            block_row.append(jnp.where(r < rows_ref[0, h], block, -1))
    block_row = jnp.concatenate(block_row, axis=1)
    for b in range(blocks):
        lanes = slice(b * cells, (b + 1) * cells)
        onehot[lanes, :] = base[...] * block_mask(block_row, b)
    ids = lax.broadcasted_iota(jnp.int32, (blocks, block_row.shape[1]), 0)
    count = lax.dot_general(
        block_mask(ids, block_row), base[...], (((1,), (1,)), ((), ())),
        preferred_element_type=F32,
    )
    keep[...] = 1.0 - 0.25 * wetf[...] * count


def ghost_onehot(halo_ghost, halo_rows, wetf, mixed):
    halo_count, depth, lanes = halo_ghost.shape[1:]
    picks = halo_count * depth * lanes
    return pl.pallas_call(
        functools.partial(ghost_kernel, halo_count=halo_count, depth=depth),
        out_shape=[vmem_out((mixed.shape[2], picks), BF16), vmem_out(wetf.shape, F32)],
        in_specs=[SMEM_SPEC, VMEM_SPEC, VMEM_SPEC, ANY_SPEC],
        out_specs=[VMEM_SPEC] * 2,
        scratch_shapes=[pltpu.VMEM((lanes, picks), BF16)],
        compiler_params=PARAMS,
        name="ghost_onehot",
    )(halo_rows, halo_ghost.reshape(halo_count * depth, lanes), *pinned(wetf, mixed))


def apply_kernel(wet_ref, keep_ref, *rest, halo_count, group):
    radius = halo_count // 2
    values = [rest[halo_order(radius).index(e)] for e in range(-radius, radius + 1) if e]
    mixed, onehot, out_hbm, staged, sems = rest[halo_count:]
    tracers, levels, ocean_cells = mixed.shape
    blocks, cells = wet_ref.shape
    span = group * cells
    picks = values[0].shape[1]

    def store(g):
        lanes = pl.ds(g * span, span)
        return pltpu.make_async_copy(
            staged.at[:, :, lanes], out_hbm.at[:, :, lanes], sems.at[g]
        )

    left = jnp.concatenate([v[...] for v in values], axis=1)
    for g in range(blocks // group):
        total = lax.dot_general(
            left,
            onehot[g * span : (g + 1) * span, :],
            (((1,), (1,)), ((), ())),
            preferred_element_type=F32,
        )
        for i in range(group):
            b = g * group + i
            lanes = slice(b * cells, (b + 1) * cells)
            here = slice(i * cells, (i + 1) * cells)
            quarter = 0.25 * wet_ref[b : b + 1, :]
            keep = keep_ref[b : b + 1, :]
            for t in range(tracers):
                staged[t, :, lanes] = (
                    mixed[t, :, lanes] * keep
                    + total[t * levels : (t + 1) * levels, here] * quarter
                )
        store(g).start()
    for g in range(blocks // group):
        store(g).wait()


def apply_halo(values, mixed, onehot, wetf, keep):
    tracers, levels, ocean_cells = mixed.shape
    halo_count = len(values)
    picks = onehot.shape[1] // halo_count
    cells = wetf.shape[1]
    blocks = ocean_cells // cells
    group = 4 if blocks % 4 == 0 else 1
    return pl.pallas_call(
        functools.partial(apply_kernel, halo_count=halo_count, group=group),
        out_shape=jax.ShapeDtypeStruct(mixed.shape, F32),
        in_specs=[VMEM_SPEC] * (halo_count + 4),
        out_specs=ANY_SPEC,
        scratch_shapes=[
            pltpu.VMEM(mixed.shape, F32),
            pltpu.SemaphoreType.DMA((blocks // group,)),
        ],
        compiler_params=PARAMS,
        name="apply_halo",
    )(*pinned(wetf, keep, *values, mixed, onehot))


def body(
    atm_flux,
    remap_send,
    remap_target,
    remap_counts,
    remap_weights,
    coupling,
    tracer,
    wet,
    mix_inverse,
    halo_send,
    halo_ghost,
    halo_rows,
):
    offsets = remap_send.shape[1]
    radius = offsets // 2
    cells = remap_weights.shape[-1]
    outgoing = select_blocks(remap_send, atm_flux, cells)
    pieces = [
        outgoing[d] if d == radius else shifted(outgoing[d], "patch", d - radius)
        for d in range(offsets)
    ]
    mixed0, column, onehot, wetf = premix(tracer, wet, mix_inverse, halo_send)
    ocean_flux, mixed, *halo_out = finish(
        pieces, remap_target, remap_counts, remap_weights[0], coupling, wetf, mixed0, column, onehot
    )
    halo_offsets = [e for e in range(-radius, radius + 1) if e]
    values = {}
    for e in halo_order(radius):
        values[e] = shifted(halo_out[halo_offsets.index(e)], "patch", e)
    ghosts, keep = ghost_onehot(halo_ghost, halo_rows, wetf, mixed)
    return ocean_flux, apply_halo(
        [values[e] for e in halo_order(radius)], mixed, ghosts, wetf, keep
    )


def solution(mesh):
    return jax.shard_map(
        body,
        mesh=mesh,
        in_specs=(
            P(None, "patch"),
            P("patch", None, None),
            P("patch", None, None),
            P("patch", None),
            P("patch", None, None, None, None),
            P(),
            P(None, None, "patch"),
            P("patch"),
            P("patch", None, None),
            P("patch", None, None, None),
            P("patch", None, None, None),
            P("patch", None),
        ),
        out_specs=(P(None, "patch"), P(None, None, "patch")),
        check_vma=False,
    )
```

```python
import functools

import jax
import jax.numpy as jnp
from jax import lax
from jax.experimental import pallas as pl
from jax.experimental.pallas import tpu as pltpu
from jax.sharding import PartitionSpec as P

F32 = jnp.float32
BF16 = jnp.bfloat16


def shifted(array, axis, by):
    length = lax.axis_size(axis)
    return lax.ppermute(array, axis, [(i, (i + by) % length) for i in range(length)])


def start_order(radius):
    return list(range(radius, 0, -1)) + list(range(-radius, 0))


def vmem_out(shape, dtype):
    return pltpu.VMEM(shape, dtype)


def pinned(*arrays):
    return [pltpu.with_memory_space_constraint(a, pltpu.VMEM) for a in arrays]


def in_hbm(*arrays):
    return [pltpu.with_memory_space_constraint(a, pltpu.HBM) for a in arrays]


SMEM_SPEC = pl.BlockSpec(memory_space=pltpu.SMEM)
VMEM_SPEC = pl.BlockSpec(memory_space=pltpu.VMEM)
ANY_SPEC = pl.BlockSpec(memory_space=pl.ANY)
PARAMS = pltpu.CompilerParams(vmem_limit_bytes=16 * 2**20)


def select_kernel(send_ref, atm_ref, *out_refs):
    offsets, capacity = send_ref.shape[0], send_ref.shape[2]
    cells = out_refs[0].shape[-1]
    for d in range(offsets):
        for c in range(capacity):
            start = pl.multiple_of(send_ref[d, 0, c] * cells, cells)
            out_refs[d][c] = atm_ref[:, pl.ds(start, cells)]


def select_blocks(remap_send, atm_flux, cells):
    offsets, capacity = remap_send.shape[1], remap_send.shape[2]
    fluxes = atm_flux.shape[0]
    return pl.pallas_call(
        select_kernel,
        out_shape=[vmem_out((capacity, fluxes, cells), BF16)] * offsets,
        in_specs=[SMEM_SPEC, VMEM_SPEC],
        out_specs=[VMEM_SPEC] * offsets,
        compiler_params=PARAMS,
        name="select_blocks",
    )(*in_hbm(jnp.transpose(remap_send, (1, 0, 2)), atm_flux))


def split(x):
    high = x.astype(BF16)
    low = (x - high.astype(F32)).astype(BF16)
    return high, low


def lane_onehot(index_ref, cells):
    parts = []
    sub = lax.broadcasted_iota(jnp.int32, (cells, index_ref.shape[1]), 0)
    for q in range(index_ref.shape[0]):
        lane = index_ref[q : q + 1, :] & (cells - 1)
        parts.append(jnp.where(sub == lane, 1.0, 0.0).astype(BF16))
    return jnp.concatenate(parts, axis=1)


def block_mask(block_row, b):
    return jnp.where(block_row == b, 1.0, 0.0).astype(BF16)


def premix_kernel(
    wet_hbm, send_hbm, tracer_hbm, inverse_hbm, mixed, column, onehot, wetf,
    wet_ref, send_ref, base, tracer, inverse, small_sems, sems, *, cuts
):
    tracers, levels, ocean_cells = tracer.shape
    blocks, cells = wet_ref.shape
    small = (
        pltpu.make_async_copy(wet_hbm, wet_ref, small_sems.at[0]),
        pltpu.make_async_copy(send_hbm, send_ref, small_sems.at[1]),
    )
    for copy in small:
        copy.start()

    def load(g):
        first, size = cuts[g], cuts[g + 1] - cuts[g]
        lanes = pl.ds(first * cells, size * cells)
        rows = pl.ds(first, size)
        return (
            pltpu.make_async_copy(
                tracer_hbm.at[:, :, lanes], tracer.at[:, :, lanes], sems.at[0, g]
            ),
            pltpu.make_async_copy(inverse_hbm.at[rows], inverse.at[rows], sems.at[1, g]),
        )

    for g in range(len(cuts) - 1):
        for copy in load(g):
            copy.start()
    for copy in small:
        copy.wait()
    wetf[...] = wet_ref[...].astype(F32)
    base[...] = lane_onehot(send_ref, cells)
    block_row = jnp.concatenate(
        [send_ref[q : q + 1, :] // cells for q in range(send_ref.shape[0])], axis=1
    )
    for b in range(blocks):
        if b in cuts:
            for copy in load(cuts.index(b)):
                copy.wait()
        lanes = slice(b * cells, (b + 1) * cells)
        wet = wetf[b : b + 1, :]
        highs, lows, raw = [], [], []
        for t in range(tracers):
            value = tracer[t, :, lanes]
            raw.append(value)
            high, low = split(value)
            highs.append(high)
            lows.append(low)
        high = jnp.concatenate(highs, axis=1)
        low = jnp.concatenate(lows, axis=1)
        matrix = inverse[b]
        m_high, m_low = split(matrix)
        left = jnp.concatenate([m_high, m_low], axis=1)
        right = jnp.concatenate([high, high], axis=0)
        solved = jnp.dot(left, right, preferred_element_type=F32) + jnp.dot(
            m_high, low, preferred_element_type=F32
        )
        for t in range(tracers):
            mixed[t, :, lanes] = jnp.where(
                wet > 0.5, solved[:, t * cells : (t + 1) * cells], raw[t]
            )
        column[b] = jnp.broadcast_to(matrix[:, 0:1], (levels, cells))
        onehot[lanes, :] = base[...] * block_mask(block_row, b)


def premix(tracer, wet, mix_inverse, halo_send):
    tracers, levels, ocean_cells = tracer.shape
    blocks = mix_inverse.shape[0]
    cells = ocean_cells // blocks
    halo_count, depth, lanes = halo_send.shape[1:]
    picks = halo_count * depth * lanes
    cuts = (0, blocks // 4, blocks)
    return pl.pallas_call(
        functools.partial(premix_kernel, cuts=cuts),
        out_shape=[
            vmem_out(tracer.shape, F32),
            vmem_out((blocks, levels, cells), F32),
            vmem_out((ocean_cells, picks), BF16),
            vmem_out((blocks, cells), F32),
        ],
        in_specs=[ANY_SPEC] * 4,
        out_specs=[VMEM_SPEC] * 4,
        scratch_shapes=[
            pltpu.VMEM((blocks, cells), jnp.int32),
            pltpu.VMEM((halo_count * depth, lanes), jnp.int32),
            pltpu.VMEM((cells, picks), BF16),
            pltpu.VMEM(tracer.shape, F32),
            pltpu.VMEM(mix_inverse.shape, F32),
            pltpu.SemaphoreType.DMA((2,)),
            pltpu.SemaphoreType.DMA((2, len(cuts) - 1)),
        ],
        compiler_params=PARAMS,
        name="premix",
    )(
        *in_hbm(
            wet.reshape(blocks, cells),
            halo_send.reshape(halo_count * depth, lanes),
            tracer,
            mix_inverse,
        )
    )


def finish_kernel(target_vmem, count_vmem, coupling_vmem, *rest, offsets, capacity):
    radius = offsets // 2
    order = start_order(radius) + [0]
    pieces = [rest[order.index(e)] for e in range(-radius, radius + 1)]
    wet_ref, weights, mixed0, column, onehot = rest[offsets : offsets + 5]
    outs = rest[offsets + 5 :]
    flux_out, mixed = outs[:2]
    halo_count = offsets - 1
    halo_outs = outs[2 : 2 + halo_count]
    sent, acc, parts, target_ref, count_ref, coupling_ref, sems = outs[2 + halo_count :]
    tracers, levels, ocean_cells = mixed0.shape
    blocks, cells = wet_ref.shape
    fluxes = flux_out.shape[0]

    small = (
        pltpu.make_async_copy(target_vmem, target_ref, sems.at[0]),
        pltpu.make_async_copy(count_vmem, count_ref, sems.at[1]),
        pltpu.make_async_copy(coupling_vmem, coupling_ref, sems.at[2]),
    )
    for copy in small:
        copy.start()
    acc[...] = jnp.zeros_like(acc)
    for d in range(offsets):
        for c in range(capacity):
            parts[d * capacity + c] = jnp.dot(
                pieces[d][c], weights[d * capacity + c], preferred_element_type=F32
            )
    for copy in small:
        copy.wait()
    for d in range(offsets):
        for c in range(capacity):
            used = jnp.where(c < count_ref[0, d], 1.0, 0.0).astype(F32)
            start = pl.multiple_of(target_ref[d, 0, c] * cells, cells)
            acc[:, pl.ds(start, cells)] += parts[d * capacity + c] * used

    sub = lax.broadcasted_iota(jnp.int32, (fluxes, cells), 0)
    couple = []
    for t in range(tracers):
        col = jnp.zeros((fluxes, cells), F32)
        for f in range(fluxes):
            col = jnp.where(sub == f, coupling_ref[t, f], col)
        couple.append(col)

    for b in range(blocks):
        lanes = slice(b * cells, (b + 1) * cells)
        flux = acc[:, lanes] * wet_ref[b : b + 1, :]
        flux_out[:, lanes] = flux
        for t in range(tracers):
            surface = jnp.sum(couple[t] * flux, axis=0, keepdims=True)
            value = mixed0[t, :, lanes] + column[b] * surface
            mixed[t, :, lanes] = value
            sent[t * levels : (t + 1) * levels, lanes] = value.astype(BF16)

    picks = onehot.shape[1] // halo_count
    for h in range(halo_count):
        halo_outs[h][...] = jnp.dot(
            sent[...], onehot[:, h * picks : (h + 1) * picks], preferred_element_type=F32
        ).astype(BF16)


def finish(pieces, remap_target, remap_counts, remap_weights, coupling, wetf, mixed0, column, onehot):
    offsets, capacity = remap_target.shape[1:]
    tracers, levels, ocean_cells = mixed0.shape
    cells = remap_weights.shape[-1]
    blocks = ocean_cells // cells
    fluxes = pieces[0].shape[1]
    halo_count = offsets - 1
    picks = onehot.shape[1] // halo_count
    return pl.pallas_call(
        functools.partial(finish_kernel, offsets=offsets, capacity=capacity),
        out_shape=[
            vmem_out((fluxes, ocean_cells), F32),
            vmem_out(mixed0.shape, F32),
        ]
        + [vmem_out((tracers * levels, picks), BF16)] * halo_count,
        in_specs=[ANY_SPEC] * 3 + [VMEM_SPEC] * (offsets + 5),
        out_specs=[VMEM_SPEC] * (2 + halo_count),
        scratch_shapes=[
            pltpu.VMEM((tracers * levels, ocean_cells), BF16),
            pltpu.VMEM((fluxes, ocean_cells), F32),
            pltpu.VMEM((offsets * capacity, fluxes, cells), F32),
            pltpu.SMEM((offsets, 1, capacity), jnp.int32),
            pltpu.SMEM(remap_counts.shape, jnp.int32),
            pltpu.SMEM(coupling.shape, F32),
            pltpu.SemaphoreType.DMA((3,)),
        ],
        input_output_aliases={3 + offsets + 2: 1},
        compiler_params=PARAMS,
        name="finish",
    )(
        *pinned(jnp.transpose(remap_target, (1, 0, 2)), remap_counts, coupling),
        *pinned(*[pieces[e + offsets // 2] for e in start_order(offsets // 2) + [0]], wetf),
        *pinned(remap_weights.reshape(offsets * capacity, cells, cells)),
        *pinned(mixed0, column, onehot),
    )


def ghost_kernel(
    rows_ref, ghost_ref, wetf, mixed_unused, onehot, keep, base, *, halo_count, depth
):
    blocks, cells = wetf.shape
    base[...] = lane_onehot(ghost_ref, cells)
    block_row = []
    for h in range(halo_count):
        for r in range(depth):
            q = h * depth + r
            block = ghost_ref[q : q + 1, :] // cells
            block_row.append(jnp.where(r < rows_ref[0, h], block, -1))
    block_row = jnp.concatenate(block_row, axis=1)
    for b in range(blocks):
        lanes = slice(b * cells, (b + 1) * cells)
        onehot[lanes, :] = base[...] * block_mask(block_row, b)
    ids = lax.broadcasted_iota(jnp.int32, (blocks, block_row.shape[1]), 0)
    count = lax.dot_general(
        block_mask(ids, block_row), base[...], (((1,), (1,)), ((), ())),
        preferred_element_type=F32,
    )
    keep[...] = 1.0 - 0.25 * wetf[...] * count


def ghost_onehot(halo_ghost, halo_rows, wetf, mixed):
    halo_count, depth, lanes = halo_ghost.shape[1:]
    picks = halo_count * depth * lanes
    return pl.pallas_call(
        functools.partial(ghost_kernel, halo_count=halo_count, depth=depth),
        out_shape=[vmem_out((mixed.shape[2], picks), BF16), vmem_out(wetf.shape, F32)],
        in_specs=[SMEM_SPEC, VMEM_SPEC, VMEM_SPEC, ANY_SPEC],
        out_specs=[VMEM_SPEC] * 2,
        scratch_shapes=[pltpu.VMEM((lanes, picks), BF16)],
        compiler_params=PARAMS,
        name="ghost_onehot",
    )(halo_rows, halo_ghost.reshape(halo_count * depth, lanes), *pinned(wetf, mixed))


def apply_kernel(wet_ref, keep_ref, *rest, halo_count, group):
    radius = halo_count // 2
    values = [rest[start_order(radius).index(e)] for e in range(-radius, radius + 1) if e]
    mixed, onehot, out_hbm, staged, sems = rest[halo_count:]
    tracers, levels, ocean_cells = mixed.shape
    blocks, cells = wet_ref.shape
    span = group * cells
    picks = values[0].shape[1]

    def store(g):
        lanes = pl.ds(g * span, span)
        return pltpu.make_async_copy(
            staged.at[:, :, lanes], out_hbm.at[:, :, lanes], sems.at[g]
        )

    left = jnp.concatenate([v[...] for v in values], axis=1)
    for g in range(blocks // group):
        total = lax.dot_general(
            left,
            onehot[g * span : (g + 1) * span, :],
            (((1,), (1,)), ((), ())),
            preferred_element_type=F32,
        )
        for i in range(group):
            b = g * group + i
            lanes = slice(b * cells, (b + 1) * cells)
            here = slice(i * cells, (i + 1) * cells)
            quarter = 0.25 * wet_ref[b : b + 1, :]
            keep = keep_ref[b : b + 1, :]
            for t in range(tracers):
                staged[t, :, lanes] = (
                    mixed[t, :, lanes] * keep
                    + total[t * levels : (t + 1) * levels, here] * quarter
                )
        store(g).start()
    for g in range(blocks // group):
        store(g).wait()


def apply_halo(values, mixed, onehot, wetf, keep):
    tracers, levels, ocean_cells = mixed.shape
    halo_count = len(values)
    picks = onehot.shape[1] // halo_count
    cells = wetf.shape[1]
    blocks = ocean_cells // cells
    group = 4 if blocks % 4 == 0 else 1
    return pl.pallas_call(
        functools.partial(apply_kernel, halo_count=halo_count, group=group),
        out_shape=jax.ShapeDtypeStruct(mixed.shape, F32),
        in_specs=[VMEM_SPEC] * (halo_count + 4),
        out_specs=ANY_SPEC,
        scratch_shapes=[
            pltpu.VMEM(mixed.shape, F32),
            pltpu.SemaphoreType.DMA((blocks // group,)),
        ],
        compiler_params=PARAMS,
        name="apply_halo",
    )(*pinned(wetf, keep, *values, mixed, onehot))


def body(
    atm_flux,
    remap_send,
    remap_target,
    remap_counts,
    remap_weights,
    coupling,
    tracer,
    wet,
    mix_inverse,
    halo_send,
    halo_ghost,
    halo_rows,
):
    offsets = remap_send.shape[1]
    radius = offsets // 2
    cells = remap_weights.shape[-1]
    outgoing = select_blocks(remap_send, atm_flux, cells)
    pieces = [
        outgoing[d] if d == radius else shifted(outgoing[d], "patch", d - radius)
        for d in range(offsets)
    ]
    mixed0, column, onehot, wetf = premix(tracer, wet, mix_inverse, halo_send)
    ocean_flux, mixed, *halo_out = finish(
        pieces, remap_target, remap_counts, remap_weights[0], coupling, wetf, mixed0, column, onehot
    )
    halo_offsets = [e for e in range(-radius, radius + 1) if e]
    values = {}
    for e in start_order(radius):
        values[e] = shifted(halo_out[halo_offsets.index(e)], "patch", e)
    ghosts, keep = ghost_onehot(halo_ghost, halo_rows, wetf, mixed)
    return ocean_flux, apply_halo(
        [values[e] for e in start_order(radius)], mixed, ghosts, wetf, keep
    )


def solution(mesh):
    return jax.shard_map(
        body,
        mesh=mesh,
        in_specs=(
            P(None, "patch"),
            P("patch", None, None),
            P("patch", None, None),
            P("patch", None),
            P("patch", None, None, None, None),
            P(),
            P(None, None, "patch"),
            P("patch"),
            P("patch", None, None),
            P("patch", None, None, None),
            P("patch", None, None, None),
            P("patch", None),
        ),
        out_specs=(P(None, "patch"), P(None, None, "patch")),
        check_vma=False,
    )
```

```python
import functools

import jax
import jax.numpy as jnp
from jax import lax
from jax.experimental import pallas as pl
from jax.experimental.pallas import tpu as pltpu
from jax.sharding import PartitionSpec as P

F32 = jnp.float32
BF16 = jnp.bfloat16


def shifted(array, axis, by):
    length = lax.axis_size(axis)
    return lax.ppermute(array, axis, [(i, (i + by) % length) for i in range(length)])


def start_order(radius):
    return list(range(radius, 0, -1)) + list(range(-radius, 0))


def vmem_out(shape, dtype):
    return pltpu.VMEM(shape, dtype)


def pinned(*arrays):
    return [pltpu.with_memory_space_constraint(a, pltpu.VMEM) for a in arrays]


def in_hbm(*arrays):
    return [pltpu.with_memory_space_constraint(a, pltpu.HBM) for a in arrays]


SMEM_SPEC = pl.BlockSpec(memory_space=pltpu.SMEM)
VMEM_SPEC = pl.BlockSpec(memory_space=pltpu.VMEM)
ANY_SPEC = pl.BlockSpec(memory_space=pl.ANY)
PARAMS = pltpu.CompilerParams(vmem_limit_bytes=16 * 2**20)


def select_kernel(send_ref, atm_ref, *out_refs):
    offsets, capacity = send_ref.shape[0], send_ref.shape[2]
    cells = out_refs[0].shape[-1]
    for d in range(offsets):
        for c in range(capacity):
            start = pl.multiple_of(send_ref[d, 0, c] * cells, cells)
            out_refs[d][c] = atm_ref[:, pl.ds(start, cells)]


def select_blocks(remap_send, atm_flux, cells):
    offsets, capacity = remap_send.shape[1], remap_send.shape[2]
    fluxes = atm_flux.shape[0]
    return pl.pallas_call(
        select_kernel,
        out_shape=[vmem_out((capacity, fluxes, cells), BF16)] * offsets,
        in_specs=[SMEM_SPEC, VMEM_SPEC],
        out_specs=[VMEM_SPEC] * offsets,
        compiler_params=PARAMS,
        name="select_blocks",
    )(*in_hbm(jnp.transpose(remap_send, (1, 0, 2)), atm_flux))


def split(x):
    high = x.astype(BF16)
    low = (x - high.astype(F32)).astype(BF16)
    return high, low


def lane_onehot(index_ref, cells):
    parts = []
    sub = lax.broadcasted_iota(jnp.int32, (cells, index_ref.shape[1]), 0)
    for q in range(index_ref.shape[0]):
        lane = index_ref[q : q + 1, :] & (cells - 1)
        parts.append(jnp.where(sub == lane, 1.0, 0.0).astype(BF16))
    return jnp.concatenate(parts, axis=1)


def block_mask(block_row, b):
    return jnp.where(block_row == b, 1.0, 0.0).astype(BF16)


def premix_kernel(
    wet_hbm, send_hbm, tracer_hbm, inverse_hbm, mixed, column, onehot, wetf,
    wet_ref, send_ref, base, tracer, inverse, small_sems, sems, *, cuts
):
    tracers, levels, ocean_cells = tracer.shape
    blocks, cells = wet_ref.shape
    small = (
        pltpu.make_async_copy(wet_hbm, wet_ref, small_sems.at[0]),
        pltpu.make_async_copy(send_hbm, send_ref, small_sems.at[1]),
    )
    for copy in small:
        copy.start()

    def load(g):
        first, size = cuts[g], cuts[g + 1] - cuts[g]
        lanes = pl.ds(first * cells, size * cells)
        rows = pl.ds(first, size)
        return (
            pltpu.make_async_copy(
                tracer_hbm.at[:, :, lanes], tracer.at[:, :, lanes], sems.at[0, g]
            ),
            pltpu.make_async_copy(inverse_hbm.at[rows], inverse.at[rows], sems.at[1, g]),
        )

    for copy in load(0):
        copy.start()
    for copy in small:
        copy.wait()
    wetf[...] = wet_ref[...].astype(F32)
    base[...] = lane_onehot(send_ref, cells)
    block_row = jnp.concatenate(
        [send_ref[q : q + 1, :] // cells for q in range(send_ref.shape[0])], axis=1
    )
    starts = {blocks // 4: 1, blocks * 3 // 4: 2}
    for b in range(blocks):
        if b in starts:
            for copy in load(starts[b]):
                copy.start()
        onehot[b * cells : (b + 1) * cells, :] = base[...] * block_mask(block_row, b)
    for b in range(blocks):
        if b in cuts:
            for copy in load(cuts.index(b)):
                copy.wait()
        lanes = slice(b * cells, (b + 1) * cells)
        wet = wetf[b : b + 1, :]
        highs, lows, raw = [], [], []
        for t in range(tracers):
            value = tracer[t, :, lanes]
            raw.append(value)
            high, low = split(value)
            highs.append(high)
            lows.append(low)
        high = jnp.concatenate(highs, axis=1)
        low = jnp.concatenate(lows, axis=1)
        matrix = inverse[b]
        m_high, m_low = split(matrix)
        left = jnp.concatenate([m_high, m_low], axis=1)
        right = jnp.concatenate([high, high], axis=0)
        solved = jnp.dot(left, right, preferred_element_type=F32) + jnp.dot(
            m_high, low, preferred_element_type=F32
        )
        for t in range(tracers):
            mixed[t, :, lanes] = jnp.where(
                wet > 0.5, solved[:, t * cells : (t + 1) * cells], raw[t]
            )
        column[b] = jnp.broadcast_to(matrix[:, 0:1], (levels, cells))


def premix(tracer, wet, mix_inverse, halo_send):
    tracers, levels, ocean_cells = tracer.shape
    blocks = mix_inverse.shape[0]
    cells = ocean_cells // blocks
    halo_count, depth, lanes = halo_send.shape[1:]
    picks = halo_count * depth * lanes
    cuts = (0, blocks * 3 // 8, blocks * 3 // 4, blocks)
    return pl.pallas_call(
        functools.partial(premix_kernel, cuts=cuts),
        out_shape=[
            vmem_out(tracer.shape, F32),
            vmem_out((blocks, levels, cells), F32),
            vmem_out((ocean_cells, picks), BF16),
            vmem_out((blocks, cells), F32),
        ],
        in_specs=[ANY_SPEC] * 4,
        out_specs=[VMEM_SPEC] * 4,
        scratch_shapes=[
            pltpu.VMEM((blocks, cells), jnp.int32),
            pltpu.VMEM((halo_count * depth, lanes), jnp.int32),
            pltpu.VMEM((cells, picks), BF16),
            pltpu.VMEM(tracer.shape, F32),
            pltpu.VMEM(mix_inverse.shape, F32),
            pltpu.SemaphoreType.DMA((2,)),
            pltpu.SemaphoreType.DMA((2, len(cuts) - 1)),
        ],
        compiler_params=PARAMS,
        name="premix",
    )(
        *in_hbm(
            wet.reshape(blocks, cells),
            halo_send.reshape(halo_count * depth, lanes),
            tracer,
            mix_inverse,
        )
    )


def finish_kernel(target_vmem, count_vmem, coupling_vmem, *rest, offsets, capacity):
    radius = offsets // 2
    order = start_order(radius) + [0]
    pieces = [rest[order.index(e)] for e in range(-radius, radius + 1)]
    wet_ref, weights, mixed0, column, onehot = rest[offsets : offsets + 5]
    outs = rest[offsets + 5 :]
    flux_out, mixed = outs[:2]
    halo_count = offsets - 1
    halo_outs = outs[2 : 2 + halo_count]
    sent, acc, parts, target_ref, count_ref, coupling_ref, sems = outs[2 + halo_count :]
    tracers, levels, ocean_cells = mixed0.shape
    blocks, cells = wet_ref.shape
    fluxes = flux_out.shape[0]

    small = (
        pltpu.make_async_copy(target_vmem, target_ref, sems.at[0]),
        pltpu.make_async_copy(count_vmem, count_ref, sems.at[1]),
        pltpu.make_async_copy(coupling_vmem, coupling_ref, sems.at[2]),
    )
    for copy in small:
        copy.start()
    acc[...] = jnp.zeros_like(acc)
    for d in range(offsets):
        for c in range(capacity):
            parts[d * capacity + c] = jnp.dot(
                pieces[d][c], weights[d * capacity + c], preferred_element_type=F32
            )
    for copy in small:
        copy.wait()
    for d in range(offsets):
        for c in range(capacity):
            used = jnp.where(c < count_ref[0, d], 1.0, 0.0).astype(F32)
            start = pl.multiple_of(target_ref[d, 0, c] * cells, cells)
            acc[:, pl.ds(start, cells)] += parts[d * capacity + c] * used

    sub = lax.broadcasted_iota(jnp.int32, (fluxes, cells), 0)
    couple = []
    for t in range(tracers):
        col = jnp.zeros((fluxes, cells), F32)
        for f in range(fluxes):
            col = jnp.where(sub == f, coupling_ref[t, f], col)
        couple.append(col)

    for b in range(blocks):
        lanes = slice(b * cells, (b + 1) * cells)
        flux = acc[:, lanes] * wet_ref[b : b + 1, :]
        flux_out[:, lanes] = flux
        for t in range(tracers):
            surface = jnp.sum(couple[t] * flux, axis=0, keepdims=True)
            value = mixed0[t, :, lanes] + column[b] * surface
            mixed[t, :, lanes] = value
            sent[t * levels : (t + 1) * levels, lanes] = value.astype(BF16)

    picks = onehot.shape[1] // halo_count
    for h in range(halo_count):
        halo_outs[h][...] = jnp.dot(
            sent[...], onehot[:, h * picks : (h + 1) * picks], preferred_element_type=F32
        ).astype(BF16)


def finish(pieces, remap_target, remap_counts, remap_weights, coupling, wetf, mixed0, column, onehot):
    offsets, capacity = remap_target.shape[1:]
    tracers, levels, ocean_cells = mixed0.shape
    cells = remap_weights.shape[-1]
    blocks = ocean_cells // cells
    fluxes = pieces[0].shape[1]
    halo_count = offsets - 1
    picks = onehot.shape[1] // halo_count
    return pl.pallas_call(
        functools.partial(finish_kernel, offsets=offsets, capacity=capacity),
        out_shape=[
            vmem_out((fluxes, ocean_cells), F32),
            vmem_out(mixed0.shape, F32),
        ]
        + [vmem_out((tracers * levels, picks), BF16)] * halo_count,
        in_specs=[ANY_SPEC] * 3 + [VMEM_SPEC] * (offsets + 5),
        out_specs=[VMEM_SPEC] * (2 + halo_count),
        scratch_shapes=[
            pltpu.VMEM((tracers * levels, ocean_cells), BF16),
            pltpu.VMEM((fluxes, ocean_cells), F32),
            pltpu.VMEM((offsets * capacity, fluxes, cells), F32),
            pltpu.SMEM((offsets, 1, capacity), jnp.int32),
            pltpu.SMEM(remap_counts.shape, jnp.int32),
            pltpu.SMEM(coupling.shape, F32),
            pltpu.SemaphoreType.DMA((3,)),
        ],
        input_output_aliases={3 + offsets + 2: 1},
        compiler_params=PARAMS,
        name="finish",
    )(
        *pinned(jnp.transpose(remap_target, (1, 0, 2)), remap_counts, coupling),
        *pinned(*[pieces[e + offsets // 2] for e in start_order(offsets // 2) + [0]], wetf),
        *pinned(remap_weights.reshape(offsets * capacity, cells, cells)),
        *pinned(mixed0, column, onehot),
    )


def ghost_kernel(
    rows_ref, ghost_ref, wetf, mixed_unused, onehot, keep, base, *, halo_count, depth
):
    blocks, cells = wetf.shape
    base[...] = lane_onehot(ghost_ref, cells)
    block_row = []
    for h in range(halo_count):
        for r in range(depth):
            q = h * depth + r
            block = ghost_ref[q : q + 1, :] // cells
            block_row.append(jnp.where(r < rows_ref[0, h], block, -1))
    block_row = jnp.concatenate(block_row, axis=1)
    for b in range(blocks):
        lanes = slice(b * cells, (b + 1) * cells)
        onehot[lanes, :] = base[...] * block_mask(block_row, b)
    ids = lax.broadcasted_iota(jnp.int32, (blocks, block_row.shape[1]), 0)
    count = lax.dot_general(
        block_mask(ids, block_row), base[...], (((1,), (1,)), ((), ())),
        preferred_element_type=F32,
    )
    keep[...] = 1.0 - 0.25 * wetf[...] * count


def ghost_onehot(halo_ghost, halo_rows, wetf, mixed):
    halo_count, depth, lanes = halo_ghost.shape[1:]
    picks = halo_count * depth * lanes
    return pl.pallas_call(
        functools.partial(ghost_kernel, halo_count=halo_count, depth=depth),
        out_shape=[vmem_out((mixed.shape[2], picks), BF16), vmem_out(wetf.shape, F32)],
        in_specs=[SMEM_SPEC, VMEM_SPEC, VMEM_SPEC, ANY_SPEC],
        out_specs=[VMEM_SPEC] * 2,
        scratch_shapes=[pltpu.VMEM((lanes, picks), BF16)],
        compiler_params=PARAMS,
        name="ghost_onehot",
    )(halo_rows, halo_ghost.reshape(halo_count * depth, lanes), *pinned(wetf, mixed))


def apply_kernel(wet_ref, keep_ref, *rest, halo_count, group):
    radius = halo_count // 2
    values = [rest[start_order(radius).index(e)] for e in range(-radius, radius + 1) if e]
    mixed, onehot, out_hbm, staged, sems = rest[halo_count:]
    tracers, levels, ocean_cells = mixed.shape
    blocks, cells = wet_ref.shape
    span = group * cells
    picks = values[0].shape[1]

    def store(g):
        lanes = pl.ds(g * span, span)
        return pltpu.make_async_copy(
            staged.at[:, :, lanes], out_hbm.at[:, :, lanes], sems.at[g]
        )

    left = jnp.concatenate([v[...] for v in values], axis=1)
    for g in range(blocks // group):
        total = lax.dot_general(
            left,
            onehot[g * span : (g + 1) * span, :],
            (((1,), (1,)), ((), ())),
            preferred_element_type=F32,
        )
        for i in range(group):
            b = g * group + i
            lanes = slice(b * cells, (b + 1) * cells)
            here = slice(i * cells, (i + 1) * cells)
            quarter = 0.25 * wet_ref[b : b + 1, :]
            keep = keep_ref[b : b + 1, :]
            for t in range(tracers):
                staged[t, :, lanes] = (
                    mixed[t, :, lanes] * keep
                    + total[t * levels : (t + 1) * levels, here] * quarter
                )
        store(g).start()
    for g in range(blocks // group):
        store(g).wait()


def apply_halo(values, mixed, onehot, wetf, keep):
    tracers, levels, ocean_cells = mixed.shape
    halo_count = len(values)
    picks = onehot.shape[1] // halo_count
    cells = wetf.shape[1]
    blocks = ocean_cells // cells
    group = 4 if blocks % 4 == 0 else 1
    return pl.pallas_call(
        functools.partial(apply_kernel, halo_count=halo_count, group=group),
        out_shape=jax.ShapeDtypeStruct(mixed.shape, F32),
        in_specs=[VMEM_SPEC] * (halo_count + 4),
        out_specs=ANY_SPEC,
        scratch_shapes=[
            pltpu.VMEM(mixed.shape, F32),
            pltpu.SemaphoreType.DMA((blocks // group,)),
        ],
        compiler_params=PARAMS,
        name="apply_halo",
    )(*pinned(wetf, keep, *values, mixed, onehot))


def body(
    atm_flux,
    remap_send,
    remap_target,
    remap_counts,
    remap_weights,
    coupling,
    tracer,
    wet,
    mix_inverse,
    halo_send,
    halo_ghost,
    halo_rows,
):
    offsets = remap_send.shape[1]
    radius = offsets // 2
    cells = remap_weights.shape[-1]
    outgoing = select_blocks(remap_send, atm_flux, cells)
    pieces = [
        outgoing[d] if d == radius else shifted(outgoing[d], "patch", d - radius)
        for d in range(offsets)
    ]
    mixed0, column, onehot, wetf = premix(tracer, wet, mix_inverse, halo_send)
    ocean_flux, mixed, *halo_out = finish(
        pieces, remap_target, remap_counts, remap_weights[0], coupling, wetf, mixed0, column, onehot
    )
    halo_offsets = [e for e in range(-radius, radius + 1) if e]
    values = {}
    for e in start_order(radius):
        values[e] = shifted(halo_out[halo_offsets.index(e)], "patch", e)
    ghosts, keep = ghost_onehot(halo_ghost, halo_rows, wetf, mixed)
    return ocean_flux, apply_halo(
        [values[e] for e in start_order(radius)], mixed, ghosts, wetf, keep
    )


def solution(mesh):
    return jax.shard_map(
        body,
        mesh=mesh,
        in_specs=(
            P(None, "patch"),
            P("patch", None, None),
            P("patch", None, None),
            P("patch", None),
            P("patch", None, None, None, None),
            P(),
            P(None, None, "patch"),
            P("patch"),
            P("patch", None, None),
            P("patch", None, None, None),
            P("patch", None, None, None),
            P("patch", None),
        ),
        out_specs=(P(None, "patch"), P(None, None, "patch")),
        check_vma=False,
    )
```
